256 devices in a mesh: ctx: 16 (over z, core), grp: 16 (over x, y).
Axes of the slice: x: 4, y: 4, z: 8, core: 2. Of those that a mesh axis runs over, the one named last changes fastest.
Arguments:
- queries: bfloat16 [4096, 8192], P('ctx', 'grp'), may hold values from -27 to 27, as said below
- keys: bfloat16 [4096, 1024], P('ctx'), may hold values from -27 to 27
- values: bfloat16 [4096, 1024], P('ctx'), may hold values from -6 to 6
- out_weight: bfloat16 [8192, 8192], P('grp'), may hold values from -0.0625 to 0.0625
- span_order: int32 [32], replicated, may hold values from 0 to 31, each once
- document: int32 [4096], replicated, may hold values from 0 to 3, never falling along the last dimension, each value on 1 to 2048 neighbouring positions
Outputs:
- projected: bfloat16 [4096, 8192], P('ctx', 'grp')
The draws below stay inside these ranges and needn't reach their ends.
Inputs may be any that keep to these rules, and one draw needn't show every extreme that they name: `queries`: queries and keys are of order one, except a few rows that may be larger.
All inputs are finite; a program needn't handle non-finite values.
Results may differ from the reference program's by a relative error of at most 0.023.
Values may be sent and summed in bfloat16 or wider, within the bound.
A program may use at most 128 MiB of HBM per device.

```python
import math
import jax
import jax.numpy as jnp
import numpy as np
from jax import lax

MODEL_DIM = 8192
Q_HEADS = 64
KV_HEADS = 8
HEAD_DIM = 128
QUERY_GROUP = 8
SPAN = 128
SEQ = 4096
N_CTX = 16
N_GRP = 16


def drawn_fields(key):
    base_query = jnp.clip(jax.random.normal(jax.random.fold_in(key, 11), (SEQ, Q_HEADS * HEAD_DIM), jnp.float32), -5.0, 5.0)
    base_key = jnp.clip(jax.random.normal(jax.random.fold_in(key, 12), (SEQ, KV_HEADS * HEAD_DIM), jnp.float32), -5.0, 5.0)
    return (base_query, base_key)


def draw_queries(key, part):
    return drawn_fields(key)[0].astype(jnp.bfloat16)


def draw_keys(key, part):
    return drawn_fields(key)[1].astype(jnp.bfloat16)


def block_scale(rng, dims, shards, low, top_value):
    factor_of, own = 1.0, jax.random.fold_in(rng, 6)
    for axis_at, blocks in shards:
        heights = jnp.exp(jax.random.uniform(jax.random.fold_in(own, axis_at), (blocks,), jnp.float32, low / len(shards), top_value / len(shards)))
        factor_of = factor_of * jnp.repeat(heights, dims[axis_at] // blocks).reshape([-1 if axis == axis_at else 1 for axis in range(len(dims))])
    return factor_of


def split_up(count, total, limit, skew):
    loads = [(1 << 20) // math.isqrt(rank ** skew) + 1 for rank in range(2, count + 1)]
    rest, counts = total - limit - (count - 1), [1] * (count - 1)
    while rest > 0:
        movable = [i for i in range(count - 1) if counts[i] < limit]
        mass, budget = sum([loads[i] for i in movable]), rest
        for i in movable:
            more = min(limit - counts[i], max(1, budget * loads[i] // mass), rest)
            counts[i] = counts[i] + more
            rest = rest - more
    return np.array([limit] + counts)


def ragged_sizes(own_key, number_of, total, reach, lean):
    if number_of == 2:
        one = jax.random.randint(own_key, (), max(1, total - reach), min(reach, total - 1) + 1)
        return jnp.stack([one, total - one])
    sizes = jnp.asarray(split_up(number_of, total, reach, lean), jnp.int32)
    twos = (number_of - 1) // 2
    donor, sink = sizes[1:1 + 2 * twos:2], sizes[2:2 + 2 * twos:2]
    slack = jnp.minimum(donor - 1, reach - sink)
    passed = jax.random.randint(jax.random.fold_in(own_key, 1), (twos,), 0, 1 << 20) % (slack + 1)
    sizes = sizes.at[1:1 + 2 * twos:2].set(donor - passed).at[2:2 + 2 * twos:2].set(sink + passed)
    return sizes[jax.random.permutation(jax.random.fold_in(own_key, 2), number_of)]


def bell_draw(own_key, dims, deviation, limit, cuts=(), kind=jnp.bfloat16):
    entries = deviation * jax.random.normal(own_key, dims, jnp.float32)
    if cuts:
        entries = entries * block_scale(own_key, dims, cuts, -0.22, 0.18)
    return jnp.clip(entries, -limit, limit).astype(kind)


def setup_inputs(seed: int = 0) -> dict:
    seeds = jax.random.split(jax.random.key(seed), 7)
    queries = draw_queries(jax.random.fold_in(seeds[6], 71), 0)
    keys = draw_keys(jax.random.fold_in(seeds[6], 71), 0)
    values = bell_draw(seeds[2], (SEQ, KV_HEADS * HEAD_DIM), 1.0, 6.0, ((0, 16),))
    out_weight = bell_draw(seeds[3], (Q_HEADS * HEAD_DIM, MODEL_DIM), (Q_HEADS * HEAD_DIM) ** -0.5, 0.0625, ((0, 16),))
    span_order = jax.random.permutation(seeds[4], 2 * N_CTX).astype(jnp.int32)
    document = jnp.searchsorted(jnp.cumsum(ragged_sizes(seeds[5], 4, SEQ, SEQ // 2, 0)), jnp.arange(SEQ), side="right").astype(jnp.int32)
    return dict(queries=queries, keys=keys, values=values, out_weight=out_weight, span_order=span_order, document=document)


def row_positions(span_order):
    rows = jnp.arange(SEQ, dtype=jnp.int32)
    return (span_order[rows // SPAN] * SPAN + rows % SPAN).astype(jnp.int32)

def reference(queries, keys, values, out_weight, span_order, document):
    positions = row_positions(span_order)
    docs = document[positions]
    visible = (positions[None, :] <= positions[:, None]) & (docs[None, :] == docs[:, None])
    score_scale = 1.0 / math.sqrt(HEAD_DIM)

    def one_head(head):
        shared = head // QUERY_GROUP
        query_head = lax.dynamic_slice_in_dim(queries, head * HEAD_DIM, HEAD_DIM, 1)
        key_head = lax.dynamic_slice_in_dim(keys, shared * HEAD_DIM, HEAD_DIM, 1)
        value_head = lax.dynamic_slice_in_dim(values, shared * HEAD_DIM, HEAD_DIM, 1)
        scores = jnp.dot(query_head, key_head.T, preferred_element_type=jnp.float32) * score_scale
        scores = jnp.where(visible, scores, -jnp.inf)
        highest = lax.optimization_barrier(jnp.max(scores, axis=1, keepdims=True))
        probs = jnp.exp(scores - highest)
        total = lax.optimization_barrier(jnp.sum(probs, axis=1, keepdims=True))
        mixed = jnp.dot(probs.astype(jnp.bfloat16), value_head, preferred_element_type=jnp.float32)
        return (mixed / total).astype(jnp.bfloat16)
    attended = lax.map(one_head, jnp.arange(Q_HEADS, dtype=jnp.int32))
    block_heads = Q_HEADS // N_GRP

    def add_block(running, block):
        head_rows = lax.dynamic_slice_in_dim(attended, block * block_heads, block_heads, 0)
        weight_rows = lax.dynamic_slice_in_dim(out_weight, block * block_heads * HEAD_DIM, block_heads * HEAD_DIM, 0)
        weight_rows = weight_rows.reshape(block_heads, HEAD_DIM, MODEL_DIM)
        block_sum = jnp.einsum('hsd,hdm->sm', head_rows.astype(jnp.float32), weight_rows.astype(jnp.float32))
        rounded = lax.optimization_barrier(block_sum.astype(jnp.bfloat16))
        return (running + rounded.astype(jnp.float32), None)
    start = jnp.zeros((SEQ, MODEL_DIM), jnp.float32)
    projected, unused = lax.scan(add_block, start, jnp.arange(N_GRP, dtype=jnp.int32))
    return projected.astype(jnp.bfloat16)
```

```python
import math

import jax
import jax.numpy as jnp
from jax import lax
from jax.experimental import pallas as pl
from jax.experimental.pallas import tpu as pltpu
from jax.sharding import PartitionSpec as P

MESH = pl.DeviceIdType.MESH
F32, BF16 = jnp.float32, jnp.bfloat16
HEAD = 128
SPAN = 128
HEADS = 4
ROWS = 256
SIDE = 4
DEPTH = 8
PER = 512
HALF = PER // 2
NB = 2
RB = ROWS // 2 // NB
LOW = -1e30
TO_LOG2 = math.log2(math.e) / math.sqrt(HEAD)


def wrap(v, n):
    return lax.rem(v + n, n)


def kernel(
    span_ref, doc_ref, q_hbm, k_hbm, v_hbm, w_hbm, out_ref,
    qbuf, kbuf, vbuf, wbuf, acc, top, att, first, send1, recv1, send2, recv2,
    load_sem, z_send, z_recv, s_send, s_recv, send1_sem, recv1_sem, send2_sem, recv2_sem,
):
    ctx, grp = lax.axis_index("ctx"), lax.axis_index("grp")
    z, core = lax.div(ctx, 2), lax.rem(ctx, 2)
    x, y = lax.div(grp, SIDE), lax.rem(grp, SIDE)
    other = 2 * z + 1 - core
    z_next = [{"ctx": 2 * wrap(z + s, DEPTH) + core} for s in (1, -1)]
    x_next = [{"grp": wrap(x + s, SIDE) * SIDE + y} for s in (1, -1)]
    y_next = [{"grp": x * SIDE + wrap(y + s, SIDE)} for s in (1, -1)]
    sibling = {"ctx": other}

    barrier = pltpu.get_barrier_semaphore()
    for there in z_next + x_next + y_next + [sibling]:
        pl.semaphore_signal(barrier, inc=1, device_id=there, device_id_type=MESH)

    head_cols = pl.ds(pl.multiple_of(lax.div(grp, 2) * HEAD, HEAD), HEAD)
    load_k = pltpu.make_async_copy(k_hbm.at[:, head_cols], kbuf.at[ctx], load_sem.at[0])
    load_v = pltpu.make_async_copy(v_hbm.at[:, head_cols], vbuf.at[ctx], load_sem.at[1])
    load_k.start()
    load_v.start()
    load_q = [
        pltpu.make_async_copy(q_hbm.at[:, pl.ds(h * HEAD, HEAD)], qbuf.at[h], load_sem.at[2 + h])
        for h in range(HEADS)
    ]
    for c in load_q:
        c.start()
    load_w = [
        pltpu.make_async_copy(
            w_hbm.at[pl.ds(h * HEAD, HEAD)], wbuf.at[pl.ds(h * HEAD, HEAD)], load_sem.at[6 + h]
        )
        for h in range(HEADS)
    ]
    for c in load_w:
        c.start()

    acc[...] = jnp.zeros_like(acc)
    top[...] = jnp.full(top.shape, LOW, F32)

    def positions(slot, shape, dim):
        return (span_ref[slot] * SPAN + lax.broadcasted_iota(jnp.int32, shape, dim)).astype(F32)

    doc = doc_ref[...]
    starts = []
    for d in range(1, 4):
        before = jnp.sum(jnp.where(doc < d, 1.0, 0.0), axis=0, keepdims=True)
        starts.append(jnp.sum(before, axis=1, keepdims=True))
    for a in range(2):
        at = positions(2 * ctx + a, (SPAN, SPAN), 0)
        begin = jnp.zeros((SPAN, SPAN), F32)
        for s in starts:
            begin = jnp.maximum(begin, jnp.where(at >= s, s, 0.0))
        first[pl.ds(a * SPAN, SPAN), :] = begin

    load_k.wait()
    load_v.wait()
    pl.semaphore_wait(barrier, 7)

    bufs = (kbuf, vbuf)

    def to_sibling(slot, step, kv):
        return pltpu.make_async_remote_copy(
            src_ref=bufs[kv].at[slot], dst_ref=bufs[kv].at[slot],
            send_sem=s_send.at[step, kv], recv_sem=s_recv.at[step, kv],
            device_id=sibling, device_id_type=MESH,
        )

    def along_z(slot, way, step, kv):
        return pltpu.make_async_remote_copy(
            src_ref=bufs[kv].at[slot], dst_ref=bufs[kv].at[slot],
            send_sem=z_send.at[way, step, kv], recv_sem=z_recv.at[way, step, kv],
            device_id=z_next[way], device_id_type=MESH,
        )

    pending = []

    def go(copy):
        copy.start()
        pending.append(copy)

    for kv in range(2):
        for way in range(2):
            go(along_z(ctx, way, 0, kv))
        go(to_sibling(ctx, 0, kv))

    for c in load_q:
        c.wait()

    def attend(zz):
        key_at = jnp.concatenate([positions(4 * zz + i, (1, SPAN), 1) for i in range(4)], axis=1)
        keys = kbuf[pl.ds(2 * zz, 2)].reshape(2 * ROWS, HEAD)
        values = vbuf[pl.ds(2 * zz, 2)].reshape(2 * ROWS, HEAD)
        values = jnp.concatenate([values, jnp.ones_like(values)], axis=1)
        hide = []
        for a in range(2):
            at = positions(2 * ctx + a, (SPAN, 4 * SPAN), 0)
            begin = jnp.concatenate([first[pl.ds(a * SPAN, SPAN), :]] * 4, axis=1)
            seen = (key_at <= at) & (key_at >= begin)
            hide.append(jnp.where(seen, 0.0, LOW))
        hide = jnp.concatenate(hide, axis=0)
        for h in range(HEADS):
            s = lax.dot_general(
                qbuf[h], keys, (((1,), (1,)), ((), ())), preferred_element_type=F32
            )
            s = s * TO_LOG2 + hide
            old = top[h]
            new = jnp.maximum(old, jnp.max(s, axis=1, keepdims=True))
            probs = jnp.exp2(s - jnp.concatenate([new] * 4, axis=1)).astype(BF16)
            shrink = jnp.exp2(old - new)
            top[h] = new
            acc[h] = acc[h] * jnp.concatenate([shrink] * 2, axis=1) + jnp.dot(
                probs, values, preferred_element_type=F32
            )

    def slot_of(way, step):
        return 2 * wrap(z + (-step if way == 0 else step), DEPTH) + core

    for step in range(1, 5):
        for kv in range(2):
            for way in range(2):
                if step == 4 and kv != way:
                    continue
                slot = slot_of(way, step)
                along_z(slot, way, step - 1, kv).wait_recv()
                if step < 3 or (step == 3 and kv == way):
                    go(along_z(slot, way, step, kv))
                go(to_sibling(slot, step if way == 0 else step + 3, kv) if step < 4
                   else to_sibling(slot, 7, kv))
        if step == 1:
            for kv in range(2):
                to_sibling(other, 0, kv).wait_recv()
            attend(z)
        else:
            for way in range(2):
                for kv in range(2):
                    to_sibling(other, step - 1 if way == 0 else step + 2, kv).wait_recv()
                attend(wrap(z + (1 - step if way == 0 else step - 1), DEPTH))
    for kv in range(2):
        to_sibling(other, 7, kv).wait_recv()
    attend(wrap(z + 4, DEPTH))

    for h in range(HEADS):
        whole = acc[h]
        att[:, pl.ds(h * HEAD, HEAD)] = (whole[:, :HEAD] / whole[:, HEAD:]).astype(BF16)
    for c in load_w:
        c.wait()

    mine = ((x, y), (y, x))
    nexts = ((x_next, y_next), (y_next, x_next))

    def own(half, a, b, row):
        target = a * SIDE + b if half == 0 else b * SIDE + a
        col = pl.multiple_of(target * PER + half * HALF, HALF)
        return jnp.dot(
            att[pl.ds(row, RB), :], wbuf[:, pl.ds(col, HALF)], preferred_element_type=F32
        )

    def row_of(side, batch):
        return side * (ROWS // 2) + batch * RB

    def side_of(way, kind):
        return 1 - way if kind == 1 else way

    def copy1(half, batch, way, kind):
        at = ((half * NB + batch) * 2 + way) * 3 + kind
        return pltpu.make_async_remote_copy(
            src_ref=send1.at[at], dst_ref=recv1.at[at],
            send_sem=send1_sem.at[at], recv_sem=recv1_sem.at[at],
            device_id=nexts[half][0][way], device_id_type=MESH,
        )

    def copy2(half, batch, way, kind):
        at = ((half * NB + batch) * 2 + way) * 3 + kind
        return pltpu.make_async_remote_copy(
            src_ref=send2.at[at], dst_ref=recv2.at[at],
            send_sem=send2_sem.at[at], recv_sem=recv2_sem.at[at],
            device_id=nexts[half][1][way], device_id_type=MESH,
        )

    def index(half, batch, way, kind):
        return ((half * NB + batch) * 2 + way) * 3 + kind

    def stage1(half, batch, way, kind):
        at = index(half, batch, way, kind)
        row = row_of(side_of(way, kind), batch)
        far = 2 if kind == 0 else 1
        a = wrap(mine[half][0] + (far if way == 0 else -far), SIDE)
        if kind == 2:
            copy1(half, batch, way, 0).wait_recv()

        def part(b, carry):
            cols = pl.ds(pl.multiple_of(b * HALF, HALF), HALF)
            value = own(half, a, b, row)
            if kind == 2:
                value = value + recv1[index(half, batch, way, 0), :, cols].astype(F32)
            send1[at, :, cols] = value.astype(BF16)
            return carry

        lax.fori_loop(0, SIDE, part, 0)
        go(copy1(half, batch, way, kind))

    def arrived1(half, batch):
        for way in range(2):
            for kind in (1, 2):
                copy1(half, batch, way, kind).wait_recv()

    def sum1(half, batch, b, side):
        value = own(half, mine[half][0], b, row_of(side, batch))
        cols = pl.ds(pl.multiple_of(b * HALF, HALF), HALF)
        for way in range(2):
            kind = 2 if way == side else 1
            value = value + recv1[index(half, batch, way, kind), :, cols].astype(F32)
        return value

    def stage2(half, batch, way, kind):
        at = index(half, batch, way, kind)
        far = 2 if kind == 0 else 1
        b = wrap(mine[half][1] + (far if way == 0 else -far), SIDE)
        value = sum1(half, batch, b, side_of(way, kind))
        if kind == 2:
            copy2(half, batch, way, 0).wait_recv()
            value = value + recv2[index(half, batch, way, 0)].astype(F32)
        send2[at] = value.astype(BF16)
        go(copy2(half, batch, way, kind))

    def finish(half, batch):
        for side in range(2):
            value = sum1(half, batch, mine[half][1], side)
            for way in range(2):
                kind = 2 if way == side else 1
                copy2(half, batch, way, kind).wait_recv()
                value = value + recv2[index(half, batch, way, kind)].astype(F32)
            out_ref[pl.ds(row_of(side, batch), RB), pl.ds(half * HALF, HALF)] = value.astype(BF16)

    def each(step, batch, kind):
        for way in range(2):
            for half in range(2):
                step(half, batch, way, kind)

    for batch in range(NB):
        each(stage1, batch, 0)
        each(stage1, batch, 1)
        if batch > 0:
            for half in range(2):
                arrived1(half, batch - 1)
            each(stage2, batch - 1, 0)
            each(stage2, batch - 1, 1)
        each(stage1, batch, 2)
        if batch > 0:
            each(stage2, batch - 1, 2)
    for half in range(2):
        arrived1(half, NB - 1)
    each(stage2, NB - 1, 0)
    each(stage2, NB - 1, 1)
    for batch in range(NB - 1):
        for half in range(2):
            finish(half, batch)
    each(stage2, NB - 1, 2)
    for half in range(2):
        finish(half, NB - 1)
    for copy in pending:
        copy.wait_send()


def shards(queries, keys, values, out_weight, span_order, document):
    count = 2 * NB * 2 * 3
    anywhere = pl.BlockSpec(memory_space=pl.ANY)
    in_vmem = pl.BlockSpec(memory_space=pltpu.VMEM)
    dma = pltpu.SemaphoreType.DMA
    return pl.pallas_call(
        kernel,
        out_shape=jax.ShapeDtypeStruct((ROWS, PER), BF16),
        in_specs=[pl.BlockSpec(memory_space=pltpu.SMEM), in_vmem] + [anywhere] * 4,
        out_specs=in_vmem,
        scratch_shapes=[
            pltpu.VMEM((HEADS, ROWS, HEAD), BF16),
            pltpu.VMEM((2 * DEPTH, ROWS, HEAD), BF16),
            pltpu.VMEM((2 * DEPTH, ROWS, HEAD), BF16),
            pltpu.VMEM((HEADS * HEAD, SIDE * SIDE * PER), BF16),
            pltpu.VMEM((HEADS, ROWS, 2 * HEAD), F32),
            pltpu.VMEM((HEADS, ROWS, HEAD), F32),
            pltpu.VMEM((ROWS, HEADS * HEAD), BF16),
            pltpu.VMEM((ROWS, HEAD), F32),
            pltpu.VMEM((count, RB, SIDE * HALF), BF16),
            pltpu.VMEM((count, RB, SIDE * HALF), BF16),
            pltpu.VMEM((count, RB, HALF), BF16),
            pltpu.VMEM((count, RB, HALF), BF16),
            dma((10,)),
            dma((2, 4, 2)),
            dma((2, 4, 2)),
            dma((8, 2)),
            dma((8, 2)),
            dma((count,)),
            dma((count,)),
            dma((count,)),
            dma((count,)),
        ],
        compiler_params=pltpu.CompilerParams(
            collective_id=0, has_side_effects=True, vmem_limit_bytes=60 * 1024 * 1024
        ),
        name="attend_project",
    )(span_order, document.reshape(32, 128), queries, keys, values, out_weight)


def solution(mesh):
    in_specs = (P("ctx", "grp"), P("ctx", None), P("ctx", None), P("grp", None), P(), P())
    return jax.shard_map(
        shards, mesh=mesh, in_specs=in_specs, out_specs=P("ctx", "grp"), check_vma=False
    )
```

```python
import math

import jax
import jax.numpy as jnp
from jax import lax
from jax.experimental import pallas as pl
from jax.experimental.pallas import tpu as pltpu
from jax.sharding import PartitionSpec as P

MESH = pl.DeviceIdType.MESH
F32, BF16 = jnp.float32, jnp.bfloat16
HEAD = 128
SPAN = 128
HEADS = 4
ROWS = 256
SIDE = 4
DEPTH = 8
PER = 512
HALF = PER // 2
SIDES = ROWS // 2
LOW = -1e30
TO_LOG2 = math.log2(math.e) / math.sqrt(HEAD)


def wrap(v, n):
    return lax.rem(v + n, n)


def kernel(
    span_ref, doc_ref, q_hbm, k_hbm, v_hbm, w_hbm, out_ref,
    qbuf, kbuf, vbuf, wbuf, acc, top, att, hide, send1, recv1, send2, recv2,
    load_sem, z_send, z_recv, s_send, s_recv, send1_sem, recv1_sem, send2_sem, recv2_sem,
):
    ctx, grp = lax.axis_index("ctx"), lax.axis_index("grp")
    z, core = lax.div(ctx, 2), lax.rem(ctx, 2)
    x, y = lax.div(grp, SIDE), lax.rem(grp, SIDE)
    other = 2 * z + 1 - core
    z_next = [{"ctx": 2 * wrap(z + s, DEPTH) + core} for s in (1, -1)]
    x_next = [{"grp": wrap(x + s, SIDE) * SIDE + y} for s in (1, -1)]
    y_next = [{"grp": x * SIDE + wrap(y + s, SIDE)} for s in (1, -1)]
    sibling = {"ctx": other}

    barrier = pltpu.get_barrier_semaphore()
    for there in z_next + x_next + y_next + [sibling]:
        pl.semaphore_signal(barrier, inc=1, device_id=there, device_id_type=MESH)

    head_cols = pl.ds(pl.multiple_of(lax.div(grp, 2) * HEAD, HEAD), HEAD)
    load_k = pltpu.make_async_copy(k_hbm.at[:, head_cols], kbuf.at[ctx], load_sem.at[0])
    load_v = pltpu.make_async_copy(v_hbm.at[:, head_cols], vbuf.at[ctx], load_sem.at[1])
    load_k.start()
    load_v.start()
    load_q = [
        pltpu.make_async_copy(q_hbm.at[:, pl.ds(h * HEAD, HEAD)], qbuf.at[h], load_sem.at[2 + h])
        for h in range(HEADS)
    ]
    for c in load_q:
        c.start()
    load_w = [
        pltpu.make_async_copy(
            w_hbm.at[pl.ds(h * HEAD, HEAD)], wbuf.at[pl.ds(h * HEAD, HEAD)], load_sem.at[6 + h]
        )
        for h in range(HEADS)
    ]
    for c in load_w:
        c.start()

    bufs = (kbuf, vbuf)

    def piece(slot, p):
        return bufs[p // 2].at[slot, pl.ds(p % 2 * SPAN, SPAN)]

    def to_sibling(slot, step, p):
        return pltpu.make_async_remote_copy(
            src_ref=piece(slot, p), dst_ref=piece(slot, p),
            send_sem=s_send.at[step, p], recv_sem=s_recv.at[step, p],
            device_id=sibling, device_id_type=MESH,
        )

    def along_z(slot, way, step, p):
        return pltpu.make_async_remote_copy(
            src_ref=piece(slot, p), dst_ref=piece(slot, p),
            send_sem=z_send.at[way, step, p], recv_sem=z_recv.at[way, step, p],
            device_id=z_next[way], device_id_type=MESH,
        )

    pending = []

    def go(copy):
        copy.start()
        pending.append(copy)

    load_k.wait()
    load_v.wait()
    pl.semaphore_wait(barrier, 7)
    for p in range(4):
        for way in range(2):
            go(along_z(ctx, way, 0, p))
    for p in range(4):
        go(to_sibling(ctx, 0, p))

    acc[...] = jnp.zeros_like(acc)
    top[...] = jnp.full(top.shape, LOW, F32)

    def positions(slot, shape, dim):
        return (span_ref[slot] * SPAN + lax.broadcasted_iota(jnp.int32, shape, dim)).astype(F32)

    doc = doc_ref[...]
    starts = []
    for d in range(1, 4):
        before = jnp.sum(jnp.where(doc < d, 1.0, 0.0), axis=0, keepdims=True)
        starts.append(jnp.sum(before, axis=1, keepdims=True))
    for a in range(2):
        at = positions(2 * ctx + a, (SPAN, SPAN), 0)
        begin = jnp.zeros((SPAN, SPAN), F32)
        for s in starts:
            begin = jnp.maximum(begin, jnp.where(at >= s, s, 0.0))

        def mask(slot, carry):
            key_at = positions(slot, (SPAN, SPAN), 1)
            seen = (key_at <= at) & (key_at >= begin)
            hide[slot // 4, pl.ds(a * SPAN, SPAN), pl.ds(pl.multiple_of(slot % 4 * SPAN, SPAN), SPAN)] = (
                jnp.where(seen, 0.0, LOW)
            )
            return carry

        lax.fori_loop(0, 4 * DEPTH, mask, 0)

    for c in load_q:
        c.wait()

    def attend(zz, h):
        keys = kbuf[pl.ds(2 * zz, 2)].reshape(2 * ROWS, HEAD)
        values = vbuf[pl.ds(2 * zz, 2)].reshape(2 * ROWS, HEAD)
        values = jnp.concatenate([values, jnp.ones_like(values)], axis=1)
        s = lax.dot_general(qbuf[h], keys, (((1,), (1,)), ((), ())), preferred_element_type=F32)
        s = s * TO_LOG2 + hide[zz]
        old = top[h]
        new = jnp.maximum(old, jnp.max(s, axis=1, keepdims=True))
        probs = jnp.exp2(s - jnp.concatenate([new] * 4, axis=1)).astype(BF16)
        shrink = jnp.exp2(old - new)
        top[h] = new
        acc[h] = acc[h] * jnp.concatenate([shrink] * 2, axis=1) + jnp.dot(
            probs, values, preferred_element_type=F32
        )

    def chip(way, step):
        return wrap(z + (-step if way == 0 else step), DEPTH)

    for step in range(1, 5):
        back = step - 1
        if back == 0:
            ready = [(z, 0)]
        else:
            ready = [(chip(way, back), back + 3 * way) for way in range(2)]
        units = [(zz, h) for h in range(HEADS) for zz, _ in ready]
        pieces = range(4) if step < 4 else range(2)
        for p in pieces:
            for way in range(2):
                q = p if step < 4 else 2 * way + p
                slot = 2 * chip(way, step) + core
                along_z(slot, way, step - 1, q).wait_recv()
                if step < 3 or (step == 3 and q // 2 == way):
                    go(along_z(slot, way, step, q))
                go(to_sibling(slot, step + 3 * way if step < 4 else 7, q))
            if p == 0:
                for _, number in ready:
                    for r in range(4):
                        to_sibling(other, number, r).wait_recv()
            share = len(units) // len(pieces)
            for zz, h in units[p * share : (p + 1) * share]:
                attend(zz, h)
    for r in range(4):
        to_sibling(other, 7, r).wait_recv()
    for h in range(HEADS):
        attend(chip(0, 4), h)

    for h in range(HEADS):
        whole = acc[h]
        att[:, pl.ds(h * HEAD, HEAD)] = (whole[:, :HEAD] / whole[:, HEAD:]).astype(BF16)
    for c in load_w:
        c.wait()

    mine = ((x, y), (y, x))
    nexts = ((x_next, y_next), (y_next, x_next))
    offsets = (2, 1, -1, 0)

    def own(half, a, j, side):
        b = wrap(mine[half][1] + offsets[j], SIDE)
        target = a * SIDE + b if half == 0 else b * SIDE + a
        col = pl.multiple_of(target * PER + half * HALF, HALF)
        return jnp.dot(
            att[pl.ds(side * SIDES, SIDES), :], wbuf[:, pl.ds(col, HALF)],
            preferred_element_type=F32,
        )

    def side_of(way, kind):
        return 1 - way if kind == 1 else way

    def at1(half, way, kind, j):
        return ((half * 2 + way) * 3 + kind) * 4 + j

    def at2(half, way, kind):
        return (half * 2 + way) * 3 + kind

    def copy1(half, way, kind, j):
        at = at1(half, way, kind, j)
        return pltpu.make_async_remote_copy(
            src_ref=send1.at[at], dst_ref=recv1.at[at],
            send_sem=send1_sem.at[at], recv_sem=recv1_sem.at[at],
            device_id=nexts[half][0][way], device_id_type=MESH,
        )

    def copy2(half, way, kind):
        at = at2(half, way, kind)
        return pltpu.make_async_remote_copy(
            src_ref=send2.at[at], dst_ref=recv2.at[at],
            send_sem=send2_sem.at[at], recv_sem=recv2_sem.at[at],
            device_id=nexts[half][1][way], device_id_type=MESH,
        )

    def stage1(half, way, kind, j):
        far = 2 if kind == 0 else 1
        a = wrap(mine[half][0] + (far if way == 0 else -far), SIDE)
        value = own(half, a, j, side_of(way, kind))
        if kind == 2:
            copy1(half, way, 0, j).wait_recv()
            value = value + recv1[at1(half, way, 0, j)].astype(F32)
        send1[at1(half, way, kind, j)] = value.astype(BF16)
        go(copy1(half, way, kind, j))

    def arrived1(half, j):
        for way in range(2):
            for kind in (1, 2):
                copy1(half, way, kind, j).wait_recv()

    def sum1(half, j, side):
        value = own(half, mine[half][0], j, side)
        for way in range(2):
            value = value + recv1[at1(half, way, 2 if way == side else 1, j)].astype(F32)
        return value

    def stage2(half, way, kind):
        value = sum1(half, 0 if kind == 0 else 1 + way, side_of(way, kind))
        if kind == 2:
            copy2(half, way, 0).wait_recv()
            value = value + recv2[at2(half, way, 0)].astype(F32)
        send2[at2(half, way, kind)] = value.astype(BF16)
        go(copy2(half, way, kind))

    def each(step, *rest):
        for way in range(2):
            for half in range(2):
                step(half, way, *rest)

    for kind in range(3):
        for j in range(4):
            each(stage1, kind, j)
    for half in range(2):
        arrived1(half, 0)
    each(stage2, 0)
    for j in (1, 2):
        for half in range(2):
            arrived1(half, j)
            stage2(half, j - 1, 1)
    each(stage2, 2)
    for half in range(2):
        arrived1(half, 3)
    for half in range(2):
        for side in range(2):
            value = sum1(half, 3, side)
            for way in range(2):
                kind = 2 if way == side else 1
                copy2(half, way, kind).wait_recv()
                value = value + recv2[at2(half, way, kind)].astype(F32)
            out_ref[pl.ds(side * SIDES, SIDES), pl.ds(half * HALF, HALF)] = value.astype(BF16)
    for copy in pending:
        copy.wait_send()


def shards(queries, keys, values, out_weight, span_order, document):
    anywhere = pl.BlockSpec(memory_space=pl.ANY)
    in_vmem = pl.BlockSpec(memory_space=pltpu.VMEM)
    dma = pltpu.SemaphoreType.DMA
    return pl.pallas_call(
        kernel,
        out_shape=jax.ShapeDtypeStruct((ROWS, PER), BF16),
        in_specs=[pl.BlockSpec(memory_space=pltpu.SMEM), in_vmem] + [anywhere] * 4,
        out_specs=in_vmem,
        scratch_shapes=[
            pltpu.VMEM((HEADS, ROWS, HEAD), BF16),
            pltpu.VMEM((2 * DEPTH, ROWS, HEAD), BF16),
            pltpu.VMEM((2 * DEPTH, ROWS, HEAD), BF16),
            pltpu.VMEM((HEADS * HEAD, SIDE * SIDE * PER), BF16),
            pltpu.VMEM((HEADS, ROWS, 2 * HEAD), F32),
            pltpu.VMEM((HEADS, ROWS, HEAD), F32),
            pltpu.VMEM((ROWS, HEADS * HEAD), BF16),
            pltpu.VMEM((DEPTH, ROWS, 4 * SPAN), F32),
            pltpu.VMEM((48, SIDES, HALF), BF16),
            pltpu.VMEM((48, SIDES, HALF), BF16),
            pltpu.VMEM((12, SIDES, HALF), BF16),
            pltpu.VMEM((12, SIDES, HALF), BF16),
            dma((10,)),
            dma((2, 4, 4)),
            dma((2, 4, 4)),
            dma((8, 4)),
            dma((8, 4)),
            dma((48,)),
            dma((48,)),
            dma((12,)),
            dma((12,)),
        ],
        compiler_params=pltpu.CompilerParams(
            collective_id=0, has_side_effects=True, vmem_limit_bytes=60 * 1024 * 1024
        ),
        name="attend_project",
    )(span_order, document.reshape(32, 128), queries, keys, values, out_weight)


def solution(mesh):
    in_specs = (P("ctx", "grp"), P("ctx", None), P("ctx", None), P("grp", None), P(), P())
    return jax.shard_map(
        shards, mesh=mesh, in_specs=in_specs, out_specs=P("ctx", "grp"), check_vma=False
    )
```
